256 devices in a mesh: groups: 2 (over z), patch: 128 (over x, y, core).
Axes of the slice: x: 8, y: 8, z: 2, core: 2. Of those that a mesh axis runs over, the one named last changes fastest.
The devices are a block of a 8x8x16 slice.
Arguments:
- queries: bfloat16 [8192, 1536], P(('groups', 'patch')), parts along dimension 0, may hold values from -8 to 8
- fresh_keys: bfloat16 [8192, 1536], P(('groups', 'patch')), parts along dimension 0, may hold values from -8 to 8
- fresh_values: bfloat16 [8192, 1536], P(('groups', 'patch')), parts along dimension 0, may hold values from -128 to 128
- stale_keys: bfloat16 [8192, 1536], P(('groups', 'patch')), parts along dimension 0, may hold values from -8 to 8
- stale_values: bfloat16 [8192, 1536], P(('groups', 'patch')), parts along dimension 0, may hold values from -128 to 128
- text_keys: bfloat16 [452, 1536], P('groups'), parts along dimension 0, may hold values from -8 to 8
- text_values: bfloat16 [452, 1536], P('groups'), parts along dimension 0, may hold values from -128 to 128
- out_weight: bfloat16 [1536, 3072], P(None, 'patch'), may hold values from -0.15625 to 0.15625
- gate_table: float32 [50, 3072], replicated, may hold values from 0.1 to 1.9
- timestep: int32 [2], P('groups'), parts along dimension 0, may hold values from 0 to 49
Outputs:
- branch: bfloat16 [8192, 3072], P(('groups', 'patch')), parts along dimension 0
The draws below stay inside these ranges and needn't reach their ends.
There are 2 independent parts, one for each index of `groups`. The reference program is written for one: setup_inputs(seed, part) draws one part's arguments, and reference() takes and returns one part's arrays. A program takes and returns all parts, laid end to end along the dimension named above; an argument that names none is the same for every part. Nothing has to cross between parts.
All inputs are finite; a program needn't handle non-finite values.
Results may differ from the reference program's by a relative error of at most 0.0095.
Values may be sent and summed in bfloat16 or wider, within the bound.
A program may use at most 128 MiB of HBM per device.

```python
import jax
import jax.numpy as jnp
from jax import lax

D = 3072
HEAD_DIM = 64
TEXT = 226
HEADS = 24
STEPS = 50
TOK_DEV = 32
TOKENS = 4096
N_PATCH = 128


def draw_queries(key, part):
    normal_part = jax.random.truncated_normal(jax.random.fold_in(key, 1), -8.0, 8.0, (TOKENS, HEADS * HEAD_DIM), jnp.float32)
    return normal_part.astype(jnp.bfloat16)


def draw_text_keys(key, part):
    normal_part = jax.random.truncated_normal(jax.random.fold_in(key, 2), -8.0, 8.0, (TEXT, HEADS * HEAD_DIM), jnp.float32)
    return normal_part.astype(jnp.bfloat16)


def shard_levels(stream_key, dims, split, least, largest):
    factor_of = 1.0
    for position, blocks in split:
        steps = jax.random.uniform(jax.random.fold_in(jax.random.fold_in(stream_key, 6), position), (blocks,), jnp.float32, least / len(split), largest / len(split))
        factor_of = factor_of * jnp.repeat(jnp.exp(steps), dims[position] // blocks).reshape((-1,) + (1,) * (len(dims) - 1 - position))
    return factor_of


def scatter_about(own_key, extent, deviation, reach, shards=(), kind=jnp.bfloat16):
    values = deviation * jax.random.normal(own_key, extent, jnp.float32)
    if shards:
        values = values * shard_levels(own_key, extent, shards, -0.22, 0.18)
    return jnp.clip(values, -reach, reach).astype(kind)


def setup_inputs(seed: int = 0, part: int = 0) -> dict:
    splits = jax.random.split(jax.random.key(seed), 11)
    part_splits = jax.random.split(jax.random.fold_in(splits[10], part), 11)
    return {
        "queries": draw_queries(jax.random.fold_in(jax.random.fold_in(splits[10], part), 71), part),
        "fresh_keys": scatter_about(part_splits[1], (TOKENS, HEADS * HEAD_DIM), 1.0, 8.0, ((0, 128),)),
        "fresh_values": scatter_about(part_splits[2], (TOKENS, HEADS * HEAD_DIM), 24.0, 128.0, ((0, 128),)),
        "stale_keys": scatter_about(part_splits[3], (TOKENS, HEADS * HEAD_DIM), 1.0, 8.0, ((0, 128),)),
        "stale_values": scatter_about(part_splits[4], (TOKENS, HEADS * HEAD_DIM), 24.0, 128.0, ((0, 128),)),
        "text_keys": draw_text_keys(jax.random.fold_in(jax.random.fold_in(splits[10], part), 71), part),
        "text_values": scatter_about(part_splits[6], (TEXT, HEADS * HEAD_DIM), 24.0, 128.0),
        "out_weight": scatter_about(splits[7], (HEADS * HEAD_DIM, D), (HEADS * HEAD_DIM) ** -0.5, 0.15625, ((1, 128),)),
        "gate_table": jnp.clip(1.0 + 0.18 * jax.random.normal(splits[8], (STEPS, D), jnp.float32), 0.1, 1.9),
        "timestep": jax.random.randint(part_splits[9], (1,), 0, STEPS).astype(jnp.int32),
    }


def reference(queries, fresh_keys, fresh_values, stale_keys, stale_values, text_keys, text_values, out_weight, gate_table, timestep):
    gating = gate_table[timestep[0]]
    scaling = HEAD_DIM ** -0.5

    def one_patch(patch_id):
        offset = (patch_id * TOK_DEV).astype(jnp.int32)
        query = lax.dynamic_slice_in_dim(queries, offset, TOK_DEV, 0).astype(jnp.float32).reshape(TOK_DEV, HEADS, HEAD_DIM)
        key_video = lax.dynamic_update_slice_in_dim(stale_keys, lax.dynamic_slice_in_dim(fresh_keys, offset, TOK_DEV, 0), offset, 0)
        value_video = lax.dynamic_update_slice_in_dim(stale_values, lax.dynamic_slice_in_dim(fresh_values, offset, TOK_DEV, 0), offset, 0)
        key_rows = jnp.concatenate([text_keys, key_video], 0).astype(jnp.float32).reshape(-1, HEADS, HEAD_DIM)
        value_rows = jnp.concatenate([text_values, value_video], 0).astype(jnp.float32).reshape(-1, HEADS, HEAD_DIM)
        scores = jnp.einsum("thd,shd->ths", query, key_rows) * scaling
        highest = jnp.max(scores, -1)
        expo = jnp.exp(scores - highest[..., None])
        total = jnp.sum(expo, -1)
        probs = lax.optimization_barrier(expo.astype(jnp.bfloat16)).astype(jnp.float32)
        weighted = jnp.einsum("ths,shd->thd", probs, value_rows)
        attended = (weighted / total[..., None]).reshape(TOK_DEV, HEADS * HEAD_DIM).astype(jnp.bfloat16)
        projected = jnp.dot(attended, out_weight, preferred_element_type=jnp.float32)
        return (projected * gating[None, :]).astype(jnp.bfloat16)

    blocks = lax.map(one_patch, jnp.arange(N_PATCH, dtype=jnp.int32))
    return blocks.reshape(TOKENS, D)
```

```python
import functools
import math

import jax
import jax.numpy as jnp
from jax import lax
from jax.experimental import pallas as pl
from jax.experimental.pallas import tpu as pltpu
from jax.sharding import PartitionSpec as P

HEAD_DIM = 64
HEADS = 24
LANES = 128
SUBS = 4
O_SUBS = 2
MESH = pl.DeviceIdType.MESH
F32 = jnp.float32
BF16 = jnp.bfloat16


def swap_halves(tile):
    return pltpu.roll(tile.astype(F32), HEAD_DIM, 1).astype(tile.dtype)


def kernel(
    side,
    q_hbm,
    fk_hbm,
    fv_hbm,
    sk_hbm,
    sv_hbm,
    tk_hbm,
    tv_hbm,
    w_hbm,
    gate_hbm,
    step_ref,
    o_ref,
    q_v,
    fk_v,
    fv_v,
    sk_v,
    sv_v,
    tk_v,
    tv_v,
    w_v,
    gate_v,
    pack_kv,
    pack_q,
    pack_f,
    kv,
    fresh,
    q_in,
    qb,
    text,
    m_s,
    l_s,
    acc,
    og,
    wg,
    wcat,
    att,
    out_send,
    out_in,
    in_sem,
    xk_s,
    xk_r,
    xq_s,
    xq_r,
    xf_s,
    xf_r,
    yk_s,
    yk_r,
    ck_s,
    ck_r,
    yw_s,
    yw_r,
    cw_s,
    cw_r,
    xo_s,
    xo_r,
    oo_s,
    oo_r,
):
    rows = q_v.shape[0]
    half_rows = rows // 2
    group = HEADS // side
    q_half = side * half_rows
    q_all = 2 * q_half
    chunk = side * rows
    sub = chunk // SUBS
    reach = side // 2
    n_text = tk_v.shape[0]
    block = w_v.shape[1] * 2 * side
    factor = HEAD_DIM ** (-0.5) * math.log2(math.e)

    me = lax.axis_index("patch")
    core = lax.rem(me, 2)
    y = lax.rem(lax.div(me, 2), side)
    x = lax.div(me, 2 * side)

    def wrap(value):
        return lax.rem(value + side, side)

    def at_x(offset):
        return {"patch": (wrap(x + offset) * side + y) * 2 + core}

    def at_y(offset):
        return {"patch": (x * side + wrap(y + offset)) * 2 + core}

    partner = {"patch": (x * side + y) * 2 + 1 - core}

    offsets = [0]
    for k in range(1, reach):
        offsets += [k, -k]
    offsets.append(reach)

    def slot_of(offset):
        return offsets.index(offset) if offset in offsets else offsets.index(offset + side)

    def remote(src, dst, send_sem, recv_sem, device):
        return pltpu.make_async_remote_copy(
            src_ref=src,
            dst_ref=dst,
            send_sem=send_sem,
            recv_sem=recv_sem,
            device_id=device,
            device_id_type=MESH,
        )

    cols_x = pl.ds(pl.multiple_of(x * block, LANES), block)
    loads = [
        pltpu.make_async_copy(src, dst, in_sem.at[i])
        for i, (src, dst) in enumerate(
            [
                (sk_hbm, sk_v),
                (sv_hbm, sv_v),
                (q_hbm, q_v),
                (fk_hbm, fk_v),
                (fv_hbm, fv_v),
                (w_hbm, w_v),
                (tk_hbm, tk_v),
                (tv_hbm, tv_v),
                (gate_hbm.at[:, cols_x], gate_v),
            ]
        )
    ]
    for load in loads:
        load.start()

    barrier = pltpu.get_barrier_semaphore()
    peers = [at_x(o) for o in offsets[1:]] + [at_y(1), at_y(-1), partner]
    for peer in peers:
        pl.semaphore_signal(barrier, inc=1, device_id=peer, device_id_type=MESH)

    def low(shape):
        return lax.broadcasted_iota(jnp.int32, shape, 1) < HEAD_DIM

    def pack_pairs(k_ref, v_ref, out):
        is_low = low((rows, LANES))
        for pair in range(HEADS // 2):
            cols = slice(pair * LANES, (pair + 1) * LANES)
            k, v = k_ref[:, cols], v_ref[:, cols]
            even, odd = 2 * pair, 2 * pair + 1
            out[even // group, even % group] = jnp.where(is_low, k, swap_halves(v))
            out[odd // group, odd % group] = jnp.where(is_low, swap_halves(k), v)

    own = y * 2 + core

    def slot_rows(slot):
        return pl.ds(slot * rows, rows)

    loads[0].wait()
    loads[1].wait()
    pack_pairs(sk_v, sv_v, pack_kv)
    pl.semaphore_wait(barrier, len(peers))

    def x_kv(offset):
        back = slot_of(-offset)
        return remote(
            pack_kv.at[wrap(x + offset)],
            kv.at[own, :, slot_rows(back), :],
            xk_s.at[slot_of(offset)],
            xk_r.at[back],
            at_x(offset),
        )

    def x_kv_wait(slot):
        remote(
            pack_kv.at[x],
            kv.at[own, :, slot_rows(slot), :],
            xk_s.at[slot],
            xk_r.at[slot],
            at_x(-offsets[slot]),
        ).wait_recv()

    for o in offsets[1:]:
        x_kv(o).start()
    kv[own, :, 0:rows, :] = pack_kv[x]

    loads[2].wait()
    is_low = low((half_rows, LANES))
    for pair in range(HEADS // 2):
        cols = slice(pair * LANES, (pair + 1) * LANES)
        top, bottom = q_v[0:half_rows, cols], q_v[half_rows:rows, cols]
        even, odd = 2 * pair, 2 * pair + 1
        pack_q[even // group, even % group] = jnp.where(is_low, top, swap_halves(bottom))
        pack_q[odd // group, odd % group] = jnp.where(is_low, swap_halves(top), bottom)

    def x_q(offset):
        return remote(
            pack_q.at[wrap(x + offset)],
            q_in.at[x],
            xq_s.at[slot_of(offset)],
            xq_r.at[slot_of(-offset)],
            at_x(offset),
        )

    loads[3].wait()
    loads[4].wait()
    pack_pairs(fk_v, fv_v, pack_f)

    def x_f(offset):
        return remote(
            pack_f.at[wrap(x + offset)],
            fresh.at[:, pl.ds(pl.multiple_of(x * rows, rows), rows), :],
            xf_s.at[slot_of(offset)],
            xf_r.at[slot_of(-offset)],
            at_x(offset),
        )

    for o in offsets[1:]:
        x_q(o).start()
    for o in offsets[1:]:
        x_f(o).start()
    q_in[x] = pack_q[x]
    fresh[:, pl.ds(pl.multiple_of(x * rows, rows), rows), :] = pack_f[x]

    loads[5].wait()
    w_cols = w_v.shape[1]
    unit = (
        lax.broadcasted_iota(jnp.int32, (w_cols, w_cols), 0)
        == lax.broadcasted_iota(jnp.int32, (w_cols, w_cols), 1)
    ).astype(BF16)
    wg[own] = lax.dot_general(
        unit, w_v[...], (((1,), (1,)), ((), ())), preferred_element_type=F32
    ).astype(BF16)

    def origin(direction, hops):
        return wrap(y - hops if direction == 0 else y + hops) * 2 + core

    def kv_piece(index, u):
        return kv.at[index, :, pl.ds(u * sub, sub), :]

    def kv_hop(direction, hops, u):
        piece = kv_piece(origin(direction, hops), u)
        return remote(
            piece,
            piece,
            yk_s.at[direction, hops, u],
            yk_r.at[direction, hops, u],
            at_y(1 if direction == 0 else -1),
        )

    def kv_arrival(direction, hops, u):
        piece = kv_piece(origin(direction, hops), u)
        remote(
            piece,
            piece,
            yk_s.at[direction, hops - 1, u],
            yk_r.at[direction, hops - 1, u],
            at_y(-1 if direction == 0 else 1),
        ).wait_recv()

    def rel(direction, hops):
        return hops if direction == 0 or hops == reach else reach + hops

    def kv_share(direction, hops, u):
        piece = kv_piece(origin(direction, hops), u)
        index = rel(direction, hops)
        return remote(piece, piece, ck_s.at[index, u], ck_r.at[index, u], partner)

    def other(direction, hops):
        return wrap(y - hops if direction == 0 else y + hops) * 2 + 1 - core

    def kv_shared(direction, hops, u):
        piece = kv_piece(other(direction, hops), u)
        index = rel(direction, hops)
        remote(piece, piece, ck_s.at[index, u], ck_r.at[index, u], partner).wait_recv()

    def carries(direction, u):
        return (u < SUBS // 2) == (direction == 0)

    def w_hop(direction, hops):
        piece = wg.at[origin(direction, hops)]
        return remote(
            piece,
            piece,
            yw_s.at[direction, hops],
            yw_r.at[direction, hops],
            at_y(1 if direction == 0 else -1),
        )

    def w_arrival(direction, hops):
        piece = wg.at[origin(direction, hops)]
        remote(
            piece,
            piece,
            yw_s.at[direction, hops - 1],
            yw_r.at[direction, hops - 1],
            at_y(-1 if direction == 0 else 1),
        ).wait_recv()

    def w_share(direction, hops):
        piece = wg.at[origin(direction, hops)]
        index = rel(direction, hops)
        return remote(piece, piece, cw_s.at[index], cw_r.at[index], partner)

    def w_shared(direction, hops):
        piece = wg.at[other(direction, hops)]
        index = rel(direction, hops)
        remote(piece, piece, cw_s.at[index], cw_r.at[index], partner).wait_recv()

    sends = []

    def go(copy):
        copy.start()
        sends.append(copy)

    go(w_hop(0, 0))
    go(w_hop(1, 0))
    go(w_share(0, 0))

    per_sub = side // SUBS
    for u in range(SUBS):
        for slot in range(u * per_sub, (u + 1) * per_sub):
            if slot:
                x_kv_wait(slot)
        go(kv_hop(0, 0, u))
        go(kv_hop(1, 0, u))
        go(kv_share(0, 0, u))

    loads[6].wait()
    loads[7].wait()
    text[:, text.shape[1] - 32 :, :] = jnp.zeros((group, 32, LANES), BF16)
    is_low_text = low((n_text, LANES))
    for i in range(group):
        head = x * group + i
        odd = jnp.broadcast_to(lax.rem(head, 2), (n_text, LANES)) == 1
        cols = pl.ds(pl.multiple_of(lax.div(head, 2) * LANES, LANES), LANES)
        k, v = tk_v[:, cols], tv_v[:, cols]
        k = jnp.where(odd, swap_halves(k), k)
        v = jnp.where(odd, v, swap_halves(v))
        text[i, 0:n_text, :] = jnp.where(is_low_text, k, v)

    def attend(pieces, keep=None, first=False):
        def one_head(i, carry):
            keys = jnp.concatenate([piece(i) for piece in pieces], axis=0)
            scores = lax.dot_general(
                qb[i], keys, (((1,), (1,)), ((), ())), preferred_element_type=F32
            )
            if keep is not None:
                scores = jnp.where(keep(scores.shape), scores, -jnp.inf)
            width = scores.shape[1] // LANES
            highest = jnp.max(scores, axis=1, keepdims=True)
            if first:
                new_m = jnp.broadcast_to(highest, (q_all, LANES))
            else:
                old_m = m_s[i]
                new_m = jnp.maximum(old_m, highest)
            expo = jnp.exp2((scores - jnp.concatenate([new_m] * width, axis=1)) * factor)
            part = expo[:, 0:LANES]
            for k in range(1, width):
                part = part + expo[:, k * LANES : (k + 1) * LANES]
            weighted = jnp.dot(expo.astype(BF16), keys, preferred_element_type=F32)
            if first:
                l_s[i] = part
                acc[i] = weighted
            else:
                shrink = jnp.exp2((old_m - new_m) * factor)
                l_s[i] = l_s[i] * shrink + part
                acc[i] = acc[i] * shrink + weighted
            m_s[i] = new_m
            return carry

        lax.fori_loop(0, group, one_head, 0)

    def start_queries():
        for slot in range(1, side):
            remote(
                pack_q.at[x],
                q_in.at[wrap(x + offsets[slot])],
                xq_s.at[slot],
                xq_r.at[slot],
                at_x(-offsets[slot]),
            ).wait_recv()
        is_low_q = low((q_half, LANES))
        for i in range(group):
            tile = jnp.concatenate([q_in[s, i] for s in range(side)], axis=0)
            zero = jnp.zeros_like(tile)
            qb[i, 0:q_half, :] = jnp.where(is_low_q, tile, zero)
            qb[i, q_half:q_all, :] = jnp.where(is_low_q, swap_halves(tile), zero)
        attend(
            [lambda i: text[i]],
            lambda shape: lax.broadcasted_iota(jnp.int32, shape, 1) < n_text,
            first=True,
        )

    def near():
        for slot in range(1, side):
            remote(
                pack_f.at[x],
                fresh.at[:, pl.ds(pl.multiple_of(wrap(x + offsets[slot]) * rows, rows), rows), :],
                xf_s.at[slot],
                xf_r.at[slot],
                at_x(-offsets[slot]),
            ).wait_recv()

        def keep(shape):
            row = lax.broadcasted_iota(jnp.int32, shape, 0)
            col = lax.broadcasted_iota(jnp.int32, shape, 1)
            patch = lax.shift_right_logical(
                jnp.bitwise_and(row, q_half - 1), half_rows.bit_length() - 1
            )
            slot = lax.shift_right_logical(col, rows.bit_length() - 1)
            far = lax.shift_right_logical(slot + 1, 1)
            source = x + jnp.where(jnp.bitwise_and(slot, 1) == 1, far, -far)
            source = jnp.where(source < 0, source + side, source)
            source = jnp.where(source >= side, source - side, source)
            stale_ok = jnp.logical_and(slot < side, source != patch)
            fresh_ok = slot - side == patch
            return jnp.logical_or(stale_ok, fresh_ok)

        attend([lambda i: kv[own, i], lambda i: fresh[i]], keep)

    def own_other():
        for u in range(SUBS):
            kv_shared(0, 0, u)
        attend([lambda i: kv[other(0, 0), i]])

    def piece_of(index, u, count):
        return lambda i: kv[index, i, u * sub : (u + count) * sub, :]

    def far(hops, u):
        def run():
            for direction in (0, 1):
                for v in (u, u + 1):
                    kv_shared(direction, hops, v)
            attend(
                [
                    piece_of(index(direction, hops), u, 2)
                    for index in (origin, other)
                    for direction in (0, 1)
                ]
            )

        return run

    def farthest():
        for u in range(SUBS):
            kv_shared(0, reach, u)
        attend([piece_of(origin(0, reach), 0, SUBS), piece_of(other(0, reach), 0, SUBS)])

    events = [(s, ((0, u), (1, u))) for s in range(1, reach) for u in range(SUBS)]
    events += [(reach, ((0, u), (1, u + SUBS // 2))) for u in range(SUBS // 2)]
    work = [(2, start_queries), (3, own_other)]
    for s in range(1, reach):
        for u in range(0, SUBS, 2):
            work.append(((s - 1) * SUBS + u + 2, far(s, u)))
    work.insert(5, (6, near))

    done = 0
    for number, (s, arrivals) in enumerate(events):
        for direction, u in arrivals:
            kv_arrival(direction, s, u)
            if s < reach and (s < reach - 1 or carries(direction, u)):
                go(kv_hop(direction, s, u))
            go(kv_share(direction, s, u))
        if done < len(work) and number >= work[done][0]:
            work[done][1]()
            done += 1
    for _, run in work[done:]:
        run()
    for direction in (0, 1):
        w_arrival(direction, 1)
        go(w_hop(direction, 1))
        go(w_share(direction, 1))
    farthest()

    is_low_o = low((q_half, LANES))
    for i in range(group):
        total = jnp.sum(l_s[i], axis=1, keepdims=True)
        attended = acc[i] / total
        top = pltpu.roll(attended[0:q_half], HEAD_DIM, 1)
        og[x, i] = jnp.where(is_low_o, top, attended[q_half:q_all]).astype(BF16)

    o_sub = q_half // O_SUBS

    def o_piece(direction, hops, u):
        return og.at[wrap(x - hops if direction == 0 else x + hops), :, pl.ds(u * o_sub, o_sub), :]

    def o_hop(direction, hops, u):
        piece = o_piece(direction, hops, u)
        return remote(
            piece,
            piece,
            xo_s.at[direction, hops, u],
            xo_r.at[direction, hops, u],
            at_x(1 if direction == 0 else -1),
        )

    def o_arrival(direction, hops, u):
        piece = o_piece(direction, hops, u)
        remote(
            piece,
            piece,
            xo_s.at[direction, hops - 1, u],
            xo_r.at[direction, hops - 1, u],
            at_x(-1 if direction == 0 else 1),
        ).wait_recv()

    def o_carries(direction, u):
        return (u < O_SUBS // 2) == (direction == 0)

    for u in range(O_SUBS):
        for direction in (0, 1):
            go(o_hop(direction, 0, u))
    early = [x_kv(o) for o in offsets[1:]] + [x_q(o) for o in offsets[1:]]
    early += [x_f(o) for o in offsets[1:]] + sends[: -2 * O_SUBS - 4]
    late = sends[-2 * O_SUBS - 4 :]
    sends = late
    for copy in early:
        copy.wait_send()

    for s in range(1, reach + 1):
        for u in range(O_SUBS):
            for direction in (0, 1):
                if s < reach or o_carries(direction, u):
                    o_arrival(direction, s, u)
                    if s < reach and (s < reach - 1 or o_carries(direction, u)):
                        go(o_hop(direction, s, u))
            if s == reach and u == 0:
                for index in range(2, side):
                    direction, hops = (0, index) if index <= reach else (1, index - reach)
                    if direction == 0:
                        w_shared(0, hops)
                    elif hops >= 2:
                        w_shared(1, hops)
                for index in range(0, 2 * side, 2):
                    pair = jnp.concatenate(
                        [wg[index].astype(F32), wg[index + 1].astype(F32)], axis=0
                    )
                    wcat[index * w_cols : (index + 2) * w_cols, :] = pair.astype(BF16)
        if s + 1 <= reach:
            for direction in (0, 1):
                if s + 1 < reach or direction == 0:
                    w_arrival(direction, s + 1)
                    if s + 1 < reach and (s + 1 < reach - 1 or direction == 0):
                        go(w_hop(direction, s + 1))
                    go(w_share(direction, s + 1))
        if s == 1:
            w_shared(0, 0)
            w_shared(0, 1)
            w_shared(1, 1)

    for pair in range(HEADS // 2):
        cols = slice(pair * LANES, (pair + 1) * LANES)
        even, odd = 2 * pair, 2 * pair + 1
        a, b = og[even // group, even % group], og[odd // group, odd % group]
        att[0:q_half, cols] = jnp.where(is_low_o, a, swap_halves(b))
        att[q_half:q_all, cols] = jnp.where(is_low_o, swap_halves(a), b)
    projected = lax.dot_general(
        att[...], wcat[...], (((1,), (1,)), ((), ())), preferred_element_type=F32
    )
    loads[8].wait()
    gating = gate_v[pl.ds(step_ref[0], 1), :]
    branch = (projected * gating).astype(BF16)
    for s in range(side):
        out_send[s, 0:half_rows, :] = branch[s * half_rows : (s + 1) * half_rows]
        out_send[s, half_rows:rows, :] = branch[
            q_half + s * half_rows : q_half + (s + 1) * half_rows
        ]

    def x_out(offset):
        return remote(
            out_send.at[wrap(x + offset)],
            out_in.at[x],
            oo_s.at[slot_of(offset)],
            oo_r.at[slot_of(-offset)],
            at_x(offset),
        )

    for o in offsets[1:]:
        go(x_out(o))
    out_in[x] = out_send[x]
    for copy in sends:
        copy.wait_send()
    for slot in range(1, side):
        remote(
            out_send.at[x],
            out_in.at[wrap(x + offsets[slot])],
            oo_s.at[slot],
            oo_r.at[slot],
            at_x(-offsets[slot]),
        ).wait_recv()
    for s in range(side):
        o_ref[:, s * block : (s + 1) * block] = out_in[s]


def solution(mesh):
    side = math.isqrt(mesh.shape["patch"] // 2)

    def body(q, fk, fv, sk, sv, tk, tv, w, gate, step):
        rows, width = q.shape
        group = HEADS // side
        chunk = side * rows
        q_half = chunk // 2
        depth, w_cols = w.shape
        block = w_cols * 2 * side
        n_text = tk.shape[0]
        text_rows = -(-n_text // LANES) * LANES
        reach = side // 2
        anywhere = pl.BlockSpec(memory_space=pl.ANY)
        dma = pltpu.SemaphoreType.DMA
        vmem = pltpu.VMEM
        return pl.pallas_call(
            functools.partial(kernel, side),
            out_shape=jax.ShapeDtypeStruct((rows, block * side), BF16),
            in_specs=[anywhere] * 9 + [pl.BlockSpec(memory_space=pltpu.SMEM)],
            out_specs=pl.BlockSpec(memory_space=pltpu.VMEM),
            scratch_shapes=[
                *[vmem((rows, width), BF16)] * 5,
                *[vmem((n_text, width), BF16)] * 2,
                vmem((depth, w_cols), BF16),
                vmem((gate.shape[0], block), F32),
                vmem((side, group, rows, LANES), BF16),
                vmem((side, group, rows // 2, LANES), BF16),
                vmem((side, group, rows, LANES), BF16),
                vmem((2 * side, group, chunk, LANES), BF16),
                vmem((group, chunk, LANES), BF16),
                vmem((side, group, rows // 2, LANES), BF16),
                vmem((group, 2 * q_half, LANES), BF16),
                vmem((group, text_rows, LANES), BF16),
                vmem((group, 2 * q_half, LANES), F32),
                vmem((group, 2 * q_half, LANES), F32),
                vmem((group, 2 * q_half, LANES), F32),
                vmem((side, group, q_half, LANES), BF16),
                vmem((2 * side, w_cols, depth), BF16),
                vmem((block, depth), BF16),
                vmem((2 * q_half, width), BF16),
                vmem((side, rows, block), BF16),
                vmem((side, rows, block), BF16),
                dma((9,)),
                *[dma((side,))] * 6,
                *[dma((2, reach, SUBS))] * 2,
                *[dma((side, SUBS))] * 2,
                *[dma((2, reach))] * 2,
                *[dma((side,))] * 2,
                *[dma((2, reach, O_SUBS))] * 2,
                *[dma((side,))] * 2,
            ],
            compiler_params=pltpu.CompilerParams(
                collective_id=0, has_side_effects=True, vmem_limit_bytes=48 * 1024 * 1024
            ),
        )(q, fk, fv, sk, sv, tk, tv, w, gate, step)

    rows_split = P(("groups", "patch"), None)
    in_specs = (rows_split,) * 5 + (P("groups", None),) * 2
    in_specs += (P(None, "patch"), P(), P("groups"))
    return jax.shard_map(body, mesh=mesh, in_specs=in_specs, out_specs=rows_split, check_vma=False)
```

```python
import functools
import math

import jax
import jax.numpy as jnp
from jax import lax
from jax.experimental import pallas as pl
from jax.experimental.pallas import tpu as pltpu
from jax.sharding import PartitionSpec as P

HEAD_DIM = 64
HEADS = 24
LANES = 128

OWN_FIRST = 6
LAG = 3
GROUPED = 4
O_SUBS = 4
MESH = pl.DeviceIdType.MESH
F32 = jnp.float32
BF16 = jnp.bfloat16


def swap_halves(tile):
    return pltpu.roll(tile.astype(F32), HEAD_DIM, 1).astype(tile.dtype)


def kernel(
    side,
    q_hbm,
    fk_hbm,
    fv_hbm,
    sk_hbm,
    sv_hbm,
    tk_hbm,
    tv_hbm,
    w_hbm,
    gate_hbm,
    step_ref,
    o_ref,
    q_v,
    fk_v,
    fv_v,
    sk_v,
    sv_v,
    tk_v,
    tv_v,
    gate_v,
    pack_kv,
    pack_q,
    pack_f,
    kv,
    fresh,
    q_in,
    qb,
    text,
    m_s,
    l_s,
    acc,
    og,
    wg,
    wcat,
    att,
    out_send,
    out_in,
    in_sem,
    xk_s,
    xk_r,
    xq_s,
    xq_r,
    xf_s,
    xf_r,
    yk_s,
    yk_r,
    ck_s,
    ck_r,
    yw_s,
    yw_r,
    cw_s,
    cw_r,
    xo_s,
    xo_r,
    oo_s,
    oo_r,
):
    rows = q_v.shape[0]
    half_rows = rows // 2
    group = HEADS // side
    q_half = side * half_rows
    q_all = 2 * q_half
    chunk = side * rows
    reach = side // 2
    subs = side
    n_text = tk_v.shape[0]
    w_cols = wg.shape[1]
    block = w_cols * 2 * side
    factor = HEAD_DIM ** (-0.5) * math.log2(math.e)

    me = lax.axis_index("patch")
    core = lax.rem(me, 2)
    y = lax.rem(lax.div(me, 2), side)
    x = lax.div(me, 2 * side)

    def wrap(value):
        return lax.rem(value + side, side)

    def at_x(offset):
        return {"patch": (wrap(x + offset) * side + y) * 2 + core}

    def at_y(offset):
        return {"patch": (x * side + wrap(y + offset)) * 2 + core}

    partner = {"patch": (x * side + y) * 2 + 1 - core}

    offsets = [0]
    for k in range(1, reach):
        offsets += [k, -k]
    offsets.append(reach)

    def slot_of(offset):
        return offsets.index(offset) if offset in offsets else offsets.index(offset + side)

    def remote(src, dst, send_sem, recv_sem, device):
        return pltpu.make_async_remote_copy(
            src_ref=src,
            dst_ref=dst,
            send_sem=send_sem,
            recv_sem=recv_sem,
            device_id=device,
            device_id_type=MESH,
        )

    own = y * 2 + core
    cols_x = pl.ds(pl.multiple_of(x * block, LANES), block)
    loads = [
        pltpu.make_async_copy(src, dst, in_sem.at[i])
        for i, (src, dst) in enumerate(
            [
                (sk_hbm, sk_v),
                (sv_hbm, sv_v),
                (q_hbm, q_v),
                (fk_hbm, fk_v),
                (fv_hbm, fv_v),
                (w_hbm, wg.at[own]),
                (tk_hbm, tk_v),
                (tv_hbm, tv_v),
                (gate_hbm.at[:, cols_x], gate_v),
            ]
        )
    ]
    for load in loads:
        load.start()

    barrier = pltpu.get_barrier_semaphore()
    peers = [at_x(o) for o in offsets[1:]] + [at_y(1), at_y(-1), partner]
    for peer in peers:
        pl.semaphore_signal(barrier, inc=1, device_id=peer, device_id_type=MESH)

    def settle(ref, sem):
        pltpu.make_async_copy(ref, ref, sem).wait()

    def low(shape):
        return lax.broadcasted_iota(jnp.int32, shape, 1) < HEAD_DIM

    def pack_pairs(k_ref, v_ref, out):
        is_low = low((rows, LANES))
        for pair in range(HEADS // 2):
            cols = slice(pair * LANES, (pair + 1) * LANES)
            k, v = k_ref[:, cols], v_ref[:, cols]
            even, odd = 2 * pair, 2 * pair + 1
            out[even // group, even % group] = jnp.where(is_low, k, swap_halves(v))
            out[odd // group, odd % group] = jnp.where(is_low, swap_halves(k), v)

    def origin(direction, hops):
        return wrap(y - hops if direction == 0 else y + hops) * 2 + core

    def kv_piece(index, u):
        return kv.at[index, u]

    def arrival_sem(direction, hops, u):
        if hops < reach - 1:
            return yk_r.at[hops * subs + u]
        return yk_r.at[hops * subs + u - (subs // 2 if direction else 0)]

    def kv_hop(direction, hops, u, source=None):
        piece = kv_piece(origin(direction, hops), u)
        return remote(
            source or piece,
            piece,
            yk_s,
            arrival_sem(direction, hops, u),
            at_y(1 if direction == 0 else -1),
        )

    def share_sem(hops, u):
        if hops == 0:
            return ck_r.at[0]
        half = u // GROUPED if hops < reach else (u % (subs // 2)) // (GROUPED // 2)
        return ck_r.at[1 + (hops - 1) * (subs // GROUPED) + half]

    def kv_share(direction, hops, u, source=None):
        piece = kv_piece(origin(direction, hops), u)
        return remote(source or piece, piece, ck_s, share_sem(hops, u), partner)

    def other(direction, hops):
        return wrap(y - hops if direction == 0 else y + hops) * 2 + 1 - core

    def carries(direction, u):
        return (u < subs // 2) == (direction == 0)

    def w_hop(direction, hops):
        piece = wg.at[origin(direction, hops)]
        return remote(piece, piece, yw_s, yw_r.at[hops], at_y(1 if direction == 0 else -1))

    def w_share(direction, hops):
        piece = wg.at[origin(direction, hops)]
        return remote(piece, piece, cw_s, cw_r, partner)

    def w_last():
        piece = wg.at[origin(0, reach - 2)]
        return remote(piece, piece, yw_s, yw_r.at[reach - 1], at_y(2))

    def w_forward(hops):
        settle(wg.at[0:2] if hops < reach else wg.at[0], yw_r.at[hops - 1])
        for direction in (0, 1):
            if hops < reach - 1:
                w_hop(direction, hops).start()
            if hops < reach or direction == 0:
                w_share(direction, hops).start()
        if hops == reach - 2:
            w_last().start()

    with jax.named_scope("load_kv"):
        loads[0].wait()
        loads[1].wait()
    with jax.named_scope("pack_kv"):
        pack_pairs(sk_v, sv_v, pack_kv)
    with jax.named_scope("barrier"):
        pl.semaphore_wait(barrier, len(peers))

    def x_kv(offset):
        back = slot_of(-offset)
        return remote(
            pack_kv.at[wrap(x + offset)],
            kv.at[own, back],
            xk_s,
            xk_r.at[back],
            at_x(offset),
        )

    def x_kv_wait(slot):
        settle(kv.at[own, slot], xk_r.at[slot])

    def own_piece(u):
        if u:
            with jax.named_scope(f"x_wait_{u}"):
                x_kv_wait(u)
        first = pack_kv.at[x] if u == 0 else None
        kv_hop(0, 0, u, first).start()
        kv_hop(1, 0, u, first).start()
        kv_share(0, 0, u, first).start()

    for o in [1, -1, reach, *offsets[3:-1]]:
        x_kv(o).start()
    own_piece(0)
    kv[own, 0] = pack_kv[x]

    loads[2].wait()
    is_low = low((half_rows, LANES))
    for pair in range(HEADS // 2):
        cols = slice(pair * LANES, (pair + 1) * LANES)
        top, bottom = q_v[0:half_rows, cols], q_v[half_rows:rows, cols]
        even, odd = 2 * pair, 2 * pair + 1
        pack_q[even // group, even % group] = jnp.where(is_low, top, swap_halves(bottom))
        pack_q[odd // group, odd % group] = jnp.where(is_low, swap_halves(top), bottom)

    def x_q(offset):
        return remote(
            pack_q.at[wrap(x + offset)],
            q_in.at[x],
            xq_s,
            xq_r,
            at_x(offset),
        )

    loads[3].wait()
    loads[4].wait()
    pack_pairs(fk_v, fv_v, pack_f)

    def x_f(offset):
        return remote(
            pack_f.at[wrap(x + offset)],
            fresh.at[x],
            xf_s,
            xf_r,
            at_x(offset),
        )

    for o in offsets[1:]:
        x_q(o).start()
    for o in offsets[1:]:
        x_f(o).start()
    q_in[x] = pack_q[x]
    fresh[x] = pack_f[x]


    loads[5].wait()
    w_hop(0, 0).start()
    w_hop(1, 0).start()
    w_share(0, 0).start()
    for u in range(1, OWN_FIRST):
        own_piece(u)

    loads[6].wait()
    loads[7].wait()
    text[:, text.shape[1] - 32 :, :] = jnp.zeros((group, 32, LANES), BF16)
    is_low_text = low((n_text, LANES))
    for i in range(group):
        head = x * group + i
        odd = jnp.broadcast_to(lax.rem(head, 2), (n_text, LANES)) == 1
        cols = pl.ds(pl.multiple_of(lax.div(head, 2) * LANES, LANES), LANES)
        k, v = tk_v[:, cols], tv_v[:, cols]
        k = jnp.where(odd, swap_halves(k), k)
        v = jnp.where(odd, v, swap_halves(v))
        text[i, 0:n_text, :] = jnp.where(is_low_text, k, v)

    def attend(pieces, keep=None, first=False):
        keys = [jnp.concatenate([p(i) for p in pieces], axis=0) for i in range(group)]
        scores = [
            lax.dot_general(qb[i], keys[i], (((1,), (1,)), ((), ())), preferred_element_type=F32)
            for i in range(group)
        ]
        if keep is not None:
            kept = keep(scores[0].shape)
            scores = [jnp.where(kept, score, -jnp.inf) for score in scores]
        width = scores[0].shape[1] // LANES
        for i in range(group):
            highest = jnp.max(scores[i], axis=1, keepdims=True)
            if first:
                new_m = jnp.broadcast_to(highest, (q_all, LANES))
            else:
                old_m = m_s[i]
                new_m = jnp.maximum(old_m, highest)
            expo = jnp.exp2((scores[i] - jnp.concatenate([new_m] * width, axis=1)) * factor)
            part = expo[:, 0:LANES]
            for k in range(1, width):
                part = part + expo[:, k * LANES : (k + 1) * LANES]
            weighted = jnp.dot(expo.astype(BF16), keys[i], preferred_element_type=F32)
            if first:
                l_s[i] = part
                acc[i] = weighted
            else:
                shrink = jnp.exp2((old_m - new_m) * factor)
                l_s[i] = l_s[i] * shrink + part
                acc[i] = acc[i] * shrink + weighted
            m_s[i] = new_m

    def start_queries():
        settle(q_in.at[1:side], xq_r)
        is_low_q = low((q_half, LANES))
        for i in range(group):
            tile = jnp.concatenate([q_in[s, i] for s in range(side)], axis=0)
            zero = jnp.zeros_like(tile)
            qb[i, 0:q_half, :] = jnp.where(is_low_q, tile, zero)
            qb[i, q_half:q_all, :] = jnp.where(is_low_q, swap_halves(tile), zero)
        attend(
            [lambda i: text[i]],
            lambda shape: lax.broadcasted_iota(jnp.int32, shape, 1) < n_text,
            first=True,
        )

    def stacked(tiles):
        return jnp.concatenate(tiles, axis=0)

    def piece_of(index, u, count):
        return lambda i: stacked([kv[index, v, i] for v in range(u, u + count)])

    def near():
        settle(pack_f.at[1:side], xf_r)

        def keep(shape):
            row = lax.broadcasted_iota(jnp.int32, shape, 0)
            col = lax.broadcasted_iota(jnp.int32, shape, 1)
            patch = lax.shift_right_logical(
                jnp.bitwise_and(row, q_half - 1), half_rows.bit_length() - 1
            )
            slot = lax.shift_right_logical(col, rows.bit_length() - 1)
            far = lax.shift_right_logical(slot + 1, 1)
            source = x + jnp.where(jnp.bitwise_and(slot, 1) == 1, far, -far)
            source = jnp.where(source < 0, source + side, source)
            source = jnp.where(source >= side, source - side, source)
            stale_ok = jnp.logical_and(slot < side, source != patch)
            fresh_ok = slot - side == patch
            return jnp.logical_or(stale_ok, fresh_ok)

        attend(
            [piece_of(own, 0, subs), lambda i: stacked([fresh[s, i] for s in range(side)])], keep
        )

    def own_other():
        settle(kv.at[0], ck_r.at[0])
        attend([piece_of(other(0, 0), 0, subs)])

    def far(hops, u):
        def run():
            settle(kv.at[0, 0 : 2 * GROUPED], share_sem(hops, u))
            attend(
                [
                    piece_of(index(direction, hops), u, GROUPED)
                    for index in (origin, other)
                    for direction in (0, 1)
                ]
            )

        return run

    def farthest(u):
        def run():
            settle(kv.at[0, 0:GROUPED], share_sem(reach, u))
            attend(
                [
                    piece_of(index(0, reach), v, GROUPED // 2)
                    for index in (origin, other)
                    for v in (u, u + subs // 2)
                ]
            )

        return run

    events = [(s, ((0, u), (1, u))) for s in range(1, reach) for u in range(subs)]
    events += [(reach, ((0, u), (1, u + subs // 2))) for u in range(subs // 2)]
    work = [(subs - 1, start_queries), (subs + LAG, own_other)]
    for s in range(1, reach):
        for u in range(0, subs, GROUPED):
            work.append(((s - 1) * subs + u + GROUPED - 1 + LAG, far(s, u)))
    work.append((2 * subs, near))
    work.append(((reach - 1) * subs + GROUPED // 2, farthest(0)))
    work = work[:1] + sorted(work[1:], key=lambda item: item[0])
    last = farthest(GROUPED // 2)
    late_own = {2 * k + 2: OWN_FIRST + k for k in range(subs - OWN_FIRST)}

    done = 0
    for number, (s, arrivals) in enumerate(events):
        if number in late_own:
            own_piece(late_own[number])
        if number == (reach - 1) * subs:
            w_forward(1)
        with jax.named_scope(f"ring_{s}_{arrivals[0][1]}"):
            settle(kv.at[0, 0:2], yk_r.at[number])
        for direction, u in arrivals:
            if s < reach and (s < reach - 1 or carries(direction, u)):
                kv_hop(direction, s, u).start()
            kv_share(direction, s, u).start()
        if done < len(work) and number >= work[done][0]:
            with jax.named_scope(f"work_{done}"):
                work[done][1]()
            done += 1
    for _, run in work[done:]:
        run()
    with jax.named_scope("farthest"):
        last()

    o_sub = q_half // O_SUBS
    is_low_o = low((q_half, LANES))
    for i in range(group):
        total = jnp.sum(l_s[i], axis=1, keepdims=True)
        attended = acc[i] / total
        top = pltpu.roll(attended[0:q_half], HEAD_DIM, 1)
        both = jnp.where(is_low_o, top, attended[q_half:q_all]).astype(BF16)
        for u in range(O_SUBS):
            og[x, u, i] = both[u * o_sub : (u + 1) * o_sub]

    def o_piece(direction, hops, u):
        return og.at[wrap(x - hops if direction == 0 else x + hops), u]

    def o_hop(direction, hops, u):
        piece = o_piece(direction, hops, u)
        return remote(
            piece, piece, xo_s, xo_r.at[hops * O_SUBS + u], at_x(1 if direction == 0 else -1)
        )

    def o_last(direction, u):
        piece = o_piece(direction, reach - 2, u)
        sem = xo_r.at[(reach - 1) * O_SUBS + u]
        return remote(piece, piece, xo_s, sem, at_x(2 if direction == 0 else -2))

    def o_carries(direction, u):
        return (u < O_SUBS // 2) == (direction == 0)

    for u in range(O_SUBS):
        for direction in (0, 1):
            o_hop(direction, 0, u).start()
    w_forward(2)
    settle(pack_kv.at[1:side], xk_s)
    settle(pack_q.at[1:side], xq_s)
    settle(pack_f.at[1:side], xf_s)
    settle(kv.at[1:side], yk_s)
    settle(kv.at[0:side], ck_s)

    for s in range(1, reach + 1):
        for u in range(O_SUBS):
            with jax.named_scope(f"o_{s}_{u}"):
                settle(og.at[0, 0 : 1 if s == reach else 2], xo_r.at[(s - 1) * O_SUBS + u])
            for direction in (0, 1):
                if s < reach - 1:
                    o_hop(direction, s, u).start()
                if s == reach - 2 and o_carries(direction, u):
                    o_last(direction, u).start()
        with jax.named_scope(f"w_{s}"):
            if s < reach - 2:
                w_forward(s + 2)
            if s == reach - 2:
                w_forward(reach)
        if s == reach - 1:
            with jax.named_scope("w_all"):
                settle(wg.at[0:side], cw_r)
                settle(wg.at[1:side], yw_s)
                settle(wg.at[0:side], cw_s)
                for index in range(0, 2 * side, 2):
                    pair = jnp.concatenate(
                        [wg[index].astype(F32), wg[index + 1].astype(F32)], axis=0
                    )
                    wcat[index * w_cols : (index + 2) * w_cols, :] = pair.astype(BF16)

    for pair in range(HEADS // 2):
        cols = slice(pair * LANES, (pair + 1) * LANES)
        even, odd = 2 * pair, 2 * pair + 1
        a, b = (
            stacked([og[h // group, u, h % group] for u in range(O_SUBS)]) for h in (even, odd)
        )
        att[0:q_half, cols] = jnp.where(is_low_o, a, swap_halves(b))
        att[q_half:q_all, cols] = jnp.where(is_low_o, swap_halves(a), b)
    projected = lax.dot_general(
        att[...], wcat[...], (((1,), (1,)), ((), ())), preferred_element_type=F32
    )
    loads[8].wait()
    gating = gate_v[pl.ds(step_ref[0], 1), :]
    branch = (projected * gating).astype(BF16)
    for s in range(side):
        out_send[s, 0:half_rows, :] = branch[s * half_rows : (s + 1) * half_rows]
        out_send[s, half_rows:rows, :] = branch[
            q_half + s * half_rows : q_half + (s + 1) * half_rows
        ]

    def x_out(offset):
        return remote(
            out_send.at[wrap(x + offset)],
            out_in.at[x],
            oo_s,
            oo_r,
            at_x(offset),
        )

    for o in offsets[:0:-1]:
        x_out(o).start()
    out_in[x] = out_send[x]
    with jax.named_scope("late"):
        settle(og.at[1:side], xo_s)
        settle(out_send.at[1:side], oo_s)
    with jax.named_scope("out_wait"):
        settle(out_in.at[1:side], oo_r)
    for s in range(side):
        o_ref[:, s * block : (s + 1) * block] = out_in[s]


def solution(mesh):
    side = math.isqrt(mesh.shape["patch"] // 2)

    def body(q, fk, fv, sk, sv, tk, tv, w, gate, step):
        w = w.T
        rows, width = q.shape
        group = HEADS // side
        chunk = side * rows
        q_half = chunk // 2
        w_cols, depth = w.shape
        block = w_cols * 2 * side
        n_text = tk.shape[0]
        text_rows = -(-n_text // LANES) * LANES
        reach, subs = side // 2, side
        anywhere = pl.BlockSpec(memory_space=pltpu.HBM)
        dma = pltpu.SemaphoreType.DMA
        vmem = pltpu.VMEM
        return pl.pallas_call(
            functools.partial(kernel, side),
            out_shape=jax.ShapeDtypeStruct((rows, block * side), BF16),
            in_specs=[anywhere] * 9 + [pl.BlockSpec(memory_space=pltpu.SMEM)],
            out_specs=pl.BlockSpec(memory_space=pltpu.VMEM),
            scratch_shapes=[
                *[vmem((rows, width), BF16)] * 5,
                *[vmem((n_text, width), BF16)] * 2,
                vmem((gate.shape[0], block), F32),
                vmem((side, group, rows, LANES), BF16),
                vmem((side, group, rows // 2, LANES), BF16),
                vmem((side, group, rows, LANES), BF16),
                vmem((2 * side, side, group, rows, LANES), BF16),
                vmem((side, group, rows, LANES), BF16),
                vmem((side, group, rows // 2, LANES), BF16),
                vmem((group, 2 * q_half, LANES), BF16),
                vmem((group, text_rows, LANES), BF16),
                vmem((group, 2 * q_half, LANES), F32),
                vmem((group, 2 * q_half, LANES), F32),
                vmem((group, 2 * q_half, LANES), F32),
                vmem((side, O_SUBS, group, q_half // O_SUBS, LANES), BF16),
                vmem((2 * side, w_cols, depth), BF16),
                vmem((block, depth), BF16),
                vmem((2 * q_half, width), BF16),
                vmem((side, rows, block), BF16),
                vmem((side, rows, block), BF16),
                dma((9,)),
                dma,
                dma((side,)),
                *[dma] * 5,
                dma(((reach - 1) * subs + subs // 2,)),
                dma,
                dma((1 + (reach - 1) * (subs // GROUPED) + 2,)),
                dma,
                dma((reach,)),
                dma,
                dma,
                dma,
                dma((reach * O_SUBS,)),
                dma,
                dma,
            ],
            compiler_params=pltpu.CompilerParams(
                collective_id=0, has_side_effects=True, vmem_limit_bytes=48 * 1024 * 1024
            ),
        )(
            *(
                pltpu.with_memory_space_constraint(a, pltpu.HBM)
                for a in (q, fk, fv, sk, sv, tk, tv, w, gate)
            ),
            step,
        )

    rows_split = P(("groups", "patch"), None)
    in_specs = (rows_split,) * 5 + (P("groups", None),) * 2
    in_specs += (P(None, "patch"), P(), P("groups"))
    return jax.shard_map(body, mesh=mesh, in_specs=in_specs, out_specs=rows_split, check_vma=False)
```

```python
import functools
import math

import jax
import jax.numpy as jnp
from jax import lax
from jax.experimental import pallas as pl
from jax.experimental.pallas import tpu as pltpu
from jax.sharding import PartitionSpec as P

HEAD_DIM = 64
HEADS = 24
LANES = 128

OWN_FIRST = 6
LAG = 3
GROUPED = 4
O_SUBS = 4
MESH = pl.DeviceIdType.MESH
F32 = jnp.float32
BF16 = jnp.bfloat16


def swap_halves(tile):
    return pltpu.roll(tile.astype(F32), HEAD_DIM, 1).astype(tile.dtype)


def kernel(
    side,
    q_hbm,
    fk_hbm,
    fv_hbm,
    sk_hbm,
    sv_hbm,
    tk_hbm,
    tv_hbm,
    w_hbm,
    gate_hbm,
    step_ref,
    o_ref,
    q_v,
    fk_v,
    fv_v,
    sk_v,
    sv_v,
    tk_v,
    tv_v,
    gate_v,
    pack_kv,
    pack_q,
    pack_f,
    kv,
    fresh,
    q_in,
    qb,
    text,
    m_s,
    l_s,
    acc,
    og,
    wg,
    wcat,
    att,
    out_send,
    in_sem,
    xk_s,
    xk_r,
    xq_s,
    xq_r,
    xf_s,
    xf_r,
    yk_s,
    yk_r,
    ck_s,
    ck_r,
    yw_s,
    yw_r,
    cw_s,
    cw_r,
    xo_s,
    xo_r,
    oo_s,
    oo_r,
):
    rows = q_v.shape[0]
    half_rows = rows // 2
    group = HEADS // side
    q_half = side * half_rows
    q_all = 2 * q_half
    chunk = side * rows
    reach = side // 2
    subs = side
    n_text = tk_v.shape[0]
    w_cols = wg.shape[1]
    block = w_cols * 2 * side
    factor = HEAD_DIM ** (-0.5) * math.log2(math.e)

    me = lax.axis_index("patch")
    core = lax.rem(me, 2)
    y = lax.rem(lax.div(me, 2), side)
    x = lax.div(me, 2 * side)

    def wrap(value):
        return lax.rem(value + side, side)

    def at_x(offset):
        return {"patch": (wrap(x + offset) * side + y) * 2 + core}

    def at_y(offset):
        return {"patch": (x * side + wrap(y + offset)) * 2 + core}

    partner = {"patch": (x * side + y) * 2 + 1 - core}

    offsets = [0]
    for k in range(1, reach):
        offsets += [k, -k]
    offsets.append(reach)

    def slot_of(offset):
        return offsets.index(offset) if offset in offsets else offsets.index(offset + side)

    def remote(src, dst, send_sem, recv_sem, device):
        return pltpu.make_async_remote_copy(
            src_ref=src,
            dst_ref=dst,
            send_sem=send_sem,
            recv_sem=recv_sem,
            device_id=device,
            device_id_type=MESH,
        )

    own = y * 2 + core
    cols_x = pl.ds(pl.multiple_of(x * block, LANES), block)
    loads = [
        pltpu.make_async_copy(src, dst, in_sem.at[i])
        for i, (src, dst) in enumerate(
            [
                (sk_hbm, sk_v),
                (sv_hbm, sv_v),
                (q_hbm, q_v),
                (fk_hbm, fk_v),
                (fv_hbm, fv_v),
                (w_hbm, wg.at[own]),
                (tk_hbm, tk_v),
                (tv_hbm, tv_v),
                (gate_hbm.at[:, cols_x], gate_v),
            ]
        )
    ]
    for load in loads[:2]:
        load.start()

    barrier = pltpu.get_barrier_semaphore()
    peers = [at_x(o) for o in offsets[:0:-1]] + [at_y(1), at_y(-1), partner]
    for peer in peers:
        pl.semaphore_signal(barrier, inc=1, device_id=peer, device_id_type=MESH)
    for load in loads[2:]:
        load.start()

    def settle(ref, sem):
        pltpu.make_async_copy(ref, ref, sem).wait()

    def low(shape):
        return lax.broadcasted_iota(jnp.int32, shape, 1) < HEAD_DIM

    def pack_pairs(k_ref, v_ref, out):
        is_low = low((rows, LANES))
        for pair in range(HEADS // 2):
            cols = slice(pair * LANES, (pair + 1) * LANES)
            k, v = k_ref[:, cols], v_ref[:, cols]
            even, odd = 2 * pair, 2 * pair + 1
            out[even // group, even % group] = jnp.where(is_low, k, swap_halves(v))
            out[odd // group, odd % group] = jnp.where(is_low, swap_halves(k), v)

    def origin(direction, hops):
        return wrap(y - hops if direction == 0 else y + hops) * 2 + core

    def kv_piece(index, u):
        return kv.at[index, u]

    def arrival_sem(direction, hops, u):
        if hops < reach - 1:
            return yk_r.at[hops * subs + u]
        return yk_r.at[hops * subs + u - (subs // 2 if direction else 0)]

    def kv_hop(direction, hops, u, source=None):
        piece = kv_piece(origin(direction, hops), u)
        return remote(
            source or piece,
            piece,
            yk_s,
            arrival_sem(direction, hops, u),
            at_y(1 if direction == 0 else -1),
        )

    def share_sem(hops, u):
        if hops == 0:
            return ck_r.at[0]
        half = u // GROUPED if hops < reach else (u % (subs // 2)) // (GROUPED // 2)
        return ck_r.at[1 + (hops - 1) * (subs // GROUPED) + half]

    def kv_share(direction, hops, u, source=None):
        piece = kv_piece(origin(direction, hops), u)
        return remote(source or piece, piece, ck_s, share_sem(hops, u), partner)

    def other(direction, hops):
        return wrap(y - hops if direction == 0 else y + hops) * 2 + 1 - core

    def carries(direction, u):
        return (u < subs // 2) == (direction == 0)

    def w_copy(direction, hops, links, lanes):
        piece = wg.at[origin(direction, hops), :, lanes]
        sem = yw_r.at[min(hops, 1)]
        return remote(piece, piece, yw_s, sem, at_y(links if direction == 0 else -links))

    def w_share(direction, hops):
        piece = wg.at[origin(direction, hops)]
        return remote(piece, piece, cw_s, cw_r, partner)

    width = wg.shape[2]
    w_halves = (pl.ds(0, width // 2), pl.ds(width // 2, width // 2))

    def w_first():
        for direction in (0, 1):
            w_copy(direction, 0, 1, pl.ds(0, width)).start()
        w_share(0, 0).start()

    def w_second():
        settle(wg.at[0:2], yw_r.at[0])
        for direction in (0, 1):
            w_copy(direction, 1, reach - 1, w_halves[direction]).start()
            for links in range(reach - 2, 0, -1):
                w_copy(direction, 1, links, pl.ds(0, width)).start()
            w_share(direction, 1).start()

    def w_third():
        settle(wg.at[0 : side - 3], yw_r.at[1])
        for hops in range(2, reach):
            for direction in (0, 1):
                w_share(direction, hops).start()
        w_share(0, reach).start()

    with jax.named_scope("load_kv"):
        loads[0].wait()
        loads[1].wait()
    with jax.named_scope("pack_kv"):
        pack_pairs(sk_v, sv_v, pack_kv)
    with jax.named_scope("barrier"):
        pl.semaphore_wait(barrier, len(peers))

    def x_kv(offset):
        back = slot_of(-offset)
        return remote(
            pack_kv.at[wrap(x + offset)],
            kv.at[own, back],
            xk_s,
            xk_r.at[back],
            at_x(offset),
        )

    def x_kv_wait(slot):
        settle(kv.at[own, slot], xk_r.at[slot])

    def own_piece(u):
        if u:
            with jax.named_scope(f"x_wait_{u}"):
                x_kv_wait(u)
        first = pack_kv.at[x] if u == 0 else None
        kv_hop(0, 0, u, first).start()
        kv_hop(1, 0, u, first).start()
        kv_share(0, 0, u, first).start()

    for o in offsets[1:]:
        x_kv(o).start()
    own_piece(0)
    kv[own, 0] = pack_kv[x]

    loads[2].wait()
    is_low = low((half_rows, LANES))
    for pair in range(HEADS // 2):
        cols = slice(pair * LANES, (pair + 1) * LANES)
        top, bottom = q_v[0:half_rows, cols], q_v[half_rows:rows, cols]
        even, odd = 2 * pair, 2 * pair + 1
        pack_q[even // group, even % group] = jnp.where(is_low, top, swap_halves(bottom))
        pack_q[odd // group, odd % group] = jnp.where(is_low, swap_halves(top), bottom)

    def x_q(offset):
        return remote(
            pack_q.at[wrap(x + offset)],
            q_in.at[x],
            xq_s,
            xq_r,
            at_x(offset),
        )

    loads[3].wait()
    loads[4].wait()
    pack_pairs(fk_v, fv_v, pack_f)

    def x_f(offset):
        return remote(
            pack_f.at[wrap(x + offset)],
            fresh.at[x],
            xf_s,
            xf_r,
            at_x(offset),
        )

    for o in offsets[1:]:
        x_q(o).start()
    for o in offsets[1:]:
        x_f(o).start()
    q_in[x] = pack_q[x]
    fresh[x] = pack_f[x]


    for u in range(1, OWN_FIRST):
        own_piece(u)

    loads[6].wait()
    loads[7].wait()
    text[:, text.shape[1] - 32 :, :] = jnp.zeros((group, 32, LANES), BF16)
    is_low_text = low((n_text, LANES))
    for i in range(group):
        head = x * group + i
        odd = jnp.broadcast_to(lax.rem(head, 2), (n_text, LANES)) == 1
        cols = pl.ds(pl.multiple_of(lax.div(head, 2) * LANES, LANES), LANES)
        k, v = tk_v[:, cols], tv_v[:, cols]
        k = jnp.where(odd, swap_halves(k), k)
        v = jnp.where(odd, v, swap_halves(v))
        text[i, 0:n_text, :] = jnp.where(is_low_text, k, v)

    def attend(pieces, keep=None, first=False):
        keys = [jnp.concatenate([p(i) for p in pieces], axis=0) for i in range(group)]
        scores = [
            lax.dot_general(qb[i], keys[i], (((1,), (1,)), ((), ())), preferred_element_type=F32)
            for i in range(group)
        ]
        if keep is not None:
            kept = keep(scores[0].shape)
            scores = [jnp.where(kept, score, -jnp.inf) for score in scores]
        width = scores[0].shape[1] // LANES
        for i in range(group):
            highest = jnp.max(scores[i], axis=1, keepdims=True)
            if first:
                new_m = jnp.broadcast_to(highest, (q_all, LANES))
            else:
                old_m = m_s[i]
                new_m = jnp.maximum(old_m, highest)
            expo = jnp.exp2((scores[i] - jnp.concatenate([new_m] * width, axis=1)) * factor)
            part = expo[:, 0:LANES]
            for k in range(1, width):
                part = part + expo[:, k * LANES : (k + 1) * LANES]
            weighted = jnp.dot(expo.astype(BF16), keys[i], preferred_element_type=F32)
            if first:
                l_s[i] = part
                acc[i] = weighted
            else:
                shrink = jnp.exp2((old_m - new_m) * factor)
                l_s[i] = l_s[i] * shrink + part
                acc[i] = acc[i] * shrink + weighted
            m_s[i] = new_m

    def start_queries():
        settle(q_in.at[1:side], xq_r)
        is_low_q = low((q_half, LANES))
        for i in range(group):
            tile = jnp.concatenate([q_in[s, i] for s in range(side)], axis=0)
            zero = jnp.zeros_like(tile)
            qb[i, 0:q_half, :] = jnp.where(is_low_q, tile, zero)
            qb[i, q_half:q_all, :] = jnp.where(is_low_q, swap_halves(tile), zero)
        attend(
            [lambda i: text[i]],
            lambda shape: lax.broadcasted_iota(jnp.int32, shape, 1) < n_text,
            first=True,
        )

    def stacked(tiles):
        return jnp.concatenate(tiles, axis=0)

    def piece_of(index, u, count):
        return lambda i: stacked([kv[index, v, i] for v in range(u, u + count)])

    def near():
        settle(pack_f.at[1:side], xf_r)

        def keep(shape):
            row = lax.broadcasted_iota(jnp.int32, shape, 0)
            col = lax.broadcasted_iota(jnp.int32, shape, 1)
            patch = lax.shift_right_logical(
                jnp.bitwise_and(row, q_half - 1), half_rows.bit_length() - 1
            )
            slot = lax.shift_right_logical(col, rows.bit_length() - 1)
            far = lax.shift_right_logical(slot + 1, 1)
            source = x + jnp.where(jnp.bitwise_and(slot, 1) == 1, far, -far)
            source = jnp.where(source < 0, source + side, source)
            source = jnp.where(source >= side, source - side, source)
            stale_ok = jnp.logical_and(slot < side, source != patch)
            fresh_ok = slot - side == patch
            return jnp.logical_or(stale_ok, fresh_ok)

        attend(
            [piece_of(own, 0, subs), lambda i: stacked([fresh[s, i] for s in range(side)])], keep
        )

    def own_other():
        settle(kv.at[0], ck_r.at[0])
        attend([piece_of(other(0, 0), 0, subs)])

    def far(hops, u):
        def run():
            settle(kv.at[0, 0 : 2 * GROUPED], share_sem(hops, u))
            attend(
                [
                    piece_of(index(direction, hops), u, GROUPED)
                    for index in (origin, other)
                    for direction in (0, 1)
                ]
            )

        return run

    def farthest(u):
        def run():
            settle(kv.at[0, 0:GROUPED], share_sem(reach, u))
            attend(
                [
                    piece_of(index(0, reach), v, GROUPED // 2)
                    for index in (origin, other)
                    for v in (u, u + subs // 2)
                ]
            )

        return run

    events = [(s, ((0, u), (1, u))) for s in range(1, reach) for u in range(subs)]
    events += [(reach, ((0, u), (1, u + subs // 2))) for u in range(subs // 2)]
    work = [(subs - 1, start_queries), (subs + LAG, own_other)]
    for s in range(1, reach):
        for u in range(0, subs, GROUPED):
            work.append(((s - 1) * subs + u + GROUPED - 1 + LAG, far(s, u)))
    work.append((2 * subs, near))
    work.append(((reach - 1) * subs + GROUPED // 2, farthest(0)))
    work = work[:1] + sorted(work[1:], key=lambda item: item[0])
    last = farthest(GROUPED // 2)
    late_own = {2 * k + 2: OWN_FIRST + k for k in range(subs - OWN_FIRST)}

    done = 0
    for number, (s, arrivals) in enumerate(events):
        if number in late_own:
            own_piece(late_own[number])
        if number == (reach - 1) * subs:
            loads[5].wait()
            w_first()
        with jax.named_scope(f"ring_{s}_{arrivals[0][1]}"):
            settle(kv.at[0, 0:2], yk_r.at[number])
        for direction, u in arrivals:
            if s < reach and (s < reach - 1 or carries(direction, u)):
                kv_hop(direction, s, u).start()
            kv_share(direction, s, u).start()
        if done < len(work) and number >= work[done][0]:
            with jax.named_scope(f"work_{done}"):
                work[done][1]()
            done += 1
    for _, run in work[done:]:
        run()
    with jax.named_scope("farthest"):
        last()

    o_sub = q_half // O_SUBS
    is_low_o = low((q_half, LANES))
    for i in range(group):
        total = jnp.sum(l_s[i], axis=1, keepdims=True)
        weighted = jnp.where(
            is_low_o, pltpu.roll(acc[i, 0:q_half], HEAD_DIM, 1), acc[i, q_half:q_all]
        )
        both = (weighted / jnp.where(is_low_o, total[0:q_half], total[q_half:q_all])).astype(BF16)
        for u in range(O_SUBS):
            og[x, u, i] = both[u * o_sub : (u + 1) * o_sub]

    def o_piece(direction, hops, u):
        return og.at[wrap(x - hops if direction == 0 else x + hops), u]

    def o_hop(direction, hops, u):
        piece = o_piece(direction, hops, u)
        return remote(
            piece, piece, xo_s, xo_r.at[hops * O_SUBS + u], at_x(1 if direction == 0 else -1)
        )

    def o_carries(direction, u):
        return (u < O_SUBS // 2) == (direction == 0)

    for u in range(O_SUBS):
        for direction in (0, 1):
            o_hop(direction, 0, u).start()
    w_second()
    settle(pack_kv.at[1:side], xk_s)
    settle(pack_q.at[1:side], xq_s)
    settle(pack_f.at[1:side], xf_s)
    settle(kv.at[1:side], yk_s)
    settle(kv.at[0:side], ck_s)

    for s in range(1, reach + 1):
        for u in range(O_SUBS):
            with jax.named_scope(f"o_{s}_{u}"):
                settle(og.at[0, 0 : 1 if s == reach else 2], xo_r.at[(s - 1) * O_SUBS + u])
            for direction in (0, 1):
                if s < reach and (s < reach - 1 or o_carries(direction, u)):
                    o_hop(direction, s, u).start()
        if s == reach - 1:
            with jax.named_scope("w_third"):
                w_third()
            with jax.named_scope("w_all"):
                settle(wg.at[0:side], cw_r)
                settle(wg.at[1:side], yw_s)
                settle(wg.at[0:side], cw_s)
                for index in range(0, 2 * side, 2):
                    pair = jnp.concatenate(
                        [wg[index].astype(F32), wg[index + 1].astype(F32)], axis=0
                    )
                    wcat[index * w_cols : (index + 2) * w_cols, :] = pair.astype(BF16)

    loads[8].wait()
    gating = gate_v[pl.ds(step_ref[0], 1), :]

    def x_out(offset):
        return remote(
            out_send.at[wrap(x + offset)], o_ref.at[:, cols_x], oo_s, oo_r, at_x(offset)
        )

    for pair in range(HEADS // 2):
        cols = slice(pair * LANES, (pair + 1) * LANES)
        even, odd = 2 * pair, 2 * pair + 1
        a, b = (
            stacked([og[h // group, u, h % group] for u in range(O_SUBS)]) for h in (even, odd)
        )
        att[0:q_half, cols] = jnp.where(is_low_o, a, swap_halves(b))
        att[q_half:q_all, cols] = jnp.where(is_low_o, swap_halves(a), b)
    projected = lax.dot_general(
        att[...], wcat[...], (((1,), (1,)), ((), ())), preferred_element_type=F32
    )
    branch = (projected * gating).astype(BF16)
    for s in range(side):
        for part in range(2):
            start = part * q_half + s * half_rows
            out_send[s, part * half_rows : (part + 1) * half_rows] = branch[
                start : start + half_rows
            ]
    for o in offsets[:0:-1]:
        x_out(o).start()
    o_ref[:, cols_x] = out_send[x]
    with jax.named_scope("late"):
        settle(og.at[1:side], xo_s)
        settle(out_send.at[1:side], oo_s)
    with jax.named_scope("out_wait"):
        settle(out_send.at[1:side], oo_r)


def solution(mesh):
    side = math.isqrt(mesh.shape["patch"] // 2)

    def body(q, fk, fv, sk, sv, tk, tv, w, gate, step):
        w = w.T
        rows, width = q.shape
        group = HEADS // side
        chunk = side * rows
        q_half = chunk // 2
        w_cols, depth = w.shape
        block = w_cols * 2 * side
        n_text = tk.shape[0]
        text_rows = -(-n_text // LANES) * LANES
        reach, subs = side // 2, side
        anywhere = pl.BlockSpec(memory_space=pltpu.HBM)
        dma = pltpu.SemaphoreType.DMA
        vmem = pltpu.VMEM
        return pl.pallas_call(
            functools.partial(kernel, side),
            out_shape=jax.ShapeDtypeStruct((rows, block * side), BF16),
            in_specs=[anywhere] * 9 + [pl.BlockSpec(memory_space=pltpu.SMEM)],
            out_specs=pl.BlockSpec(memory_space=pltpu.VMEM),
            scratch_shapes=[
                *[vmem((rows, width), BF16)] * 5,
                *[vmem((n_text, width), BF16)] * 2,
                vmem((gate.shape[0], block), F32),
                vmem((side, group, rows, LANES), BF16),
                vmem((side, group, rows // 2, LANES), BF16),
                vmem((side, group, rows, LANES), BF16),
                vmem((2 * side, side, group, rows, LANES), BF16),
                vmem((side, group, rows, LANES), BF16),
                vmem((side, group, rows // 2, LANES), BF16),
                vmem((group, 2 * q_half, LANES), BF16),
                vmem((group, text_rows, LANES), BF16),
                vmem((group, 2 * q_half, LANES), F32),
                vmem((group, 2 * q_half, LANES), F32),
                vmem((group, 2 * q_half, LANES), F32),
                vmem((side, O_SUBS, group, q_half // O_SUBS, LANES), BF16),
                vmem((2 * side, w_cols, depth), BF16),
                vmem((block, depth), BF16),
                vmem((2 * q_half, width), BF16),
                vmem((side, rows, block), BF16),
                dma((9,)),
                dma,
                dma((side,)),
                *[dma] * 5,
                dma(((reach - 1) * subs + subs // 2,)),
                dma,
                dma((1 + (reach - 1) * (subs // GROUPED) + 2,)),
                dma,
                dma((reach,)),
                dma,
                dma,
                dma,
                dma((reach * O_SUBS,)),
                dma,
                dma,
            ],
            compiler_params=pltpu.CompilerParams(
                collective_id=0, has_side_effects=True, vmem_limit_bytes=48 * 1024 * 1024
            ),
        )(
            *(
                pltpu.with_memory_space_constraint(a, pltpu.HBM)
                for a in (q, fk, fv, sk, sv, tk, tv, w, gate)
            ),
            step,
        )

    rows_split = P(("groups", "patch"), None)
    in_specs = (rows_split,) * 5 + (P("groups", None),) * 2
    in_specs += (P(None, "patch"), P(), P("groups"))
    return jax.shard_map(body, mesh=mesh, in_specs=in_specs, out_specs=rows_split, check_vma=False)
```
